32 devices in a mesh: replica: 2 (over core), dp: 16 (over z, y, x).
Axes of the slice: x: 2, y: 2, z: 4, core: 2. Of those that a mesh axis runs over, the one named last changes fastest.
Arguments:
- layer_input: bfloat16 [2, 6144, 3072], P('replica', 'dp'), may hold values from -6 to 6
- key_cotangent: bfloat16 [2, 6144, 512], P('replica', 'dp'), may hold values from -0.029907227 to 0.029907227
- local_params: float32 [2, 3072, 512], P('replica', 'dp'), may hold values from -6 to 6
- global_params: float32 [3072, 512], P('dp'), may hold values from -6 to 6
- outer_momentum: float32 [16, 192, 512], P('dp', 'replica'), may hold values from -3 to 3
- adam_first: float32 [2, 3072, 512], P('replica', 'dp'), may hold values from -2 to 2
- adam_second: float32 [2, 3072, 512], P('replica', 'dp'), may hold values from 0.25 to 4
Outputs:
- merged_params: bfloat16 [2, 3072, 512], P('replica')
- new_global: float32 [3072, 512], P('dp')
- new_momentum: float32 [16, 192, 512], P('dp', 'replica')
- new_first: float32 [2, 3072, 512], P('replica', 'dp')
- new_second: float32 [2, 3072, 512], P('replica', 'dp')
The draws below stay inside these ranges and needn't reach their ends.
All inputs are finite; a program needn't handle non-finite values.
Results may differ from the reference program's by a relative error of at most 0.0004.
Values may be sent and summed in bfloat16 or wider, within the bound.
A program may use at most 64 MiB of HBM per device.

```python
import math
import jax
import jax.numpy as jnp
from jax import lax

DW = 3072
KW = 512
TOKENS = 6144
N_REPLICA = 2
N_DP = 16


def spiked(values, own_key, source, target, shards_of, factor):
    owner, partner = [(jnp.arange(values.shape[axis_at]) // (values.shape[axis_at] // shards_of)).reshape([-1 if axis == axis_at else 1 for axis in range(values.ndim)]) for axis_at in (source, target)]
    chosen = jax.random.permutation(own_key, shards_of)[partner]
    strong = (owner == chosen) | (owner == (partner + shards_of // 2) % shards_of)
    return jnp.where(strong, factor * values, values)


def shard_levels(stream_key, dims, shards, low, largest):
    def one(position, shards_of):
        steps = jax.random.uniform(jax.random.fold_in(jax.random.fold_in(stream_key, 6), position), (shards_of,), jnp.float32, low / len(shards), largest / len(shards))
        return jnp.repeat(jnp.exp(steps), dims[position] // shards_of).reshape((-1,) + (1,) * (len(dims) - position - 1))

    loudness = one(*shards[0])
    for cut in shards[1:]:
        loudness = loudness * one(*cut)
    return loudness


def centred(stream_key, dims, scale, most, split=(), kind=jnp.bfloat16):
    values = jax.random.normal(stream_key, dims, jnp.float32) * scale
    if len(split) > 0:
        values = shard_levels(stream_key, dims, split, -0.22, 0.18) * values
    return jnp.clip(values, min=-most, max=most).astype(kind)


def gaussian_with(rng, extent, scale, limit, shards, heavy, kind=jnp.bfloat16):
    result = scale * jax.random.normal(rng, extent, jnp.float32)
    if shards:
        result = result * shard_levels(rng, extent, shards, -0.22, 0.18)
    return jnp.clip(spiked(result, jax.random.fold_in(rng, 3), *heavy), -limit, limit).astype(kind)


def setup_inputs(seed: int = 0) -> dict:
    splits = jax.random.split(jax.random.key(seed), 8)
    layer_input = gaussian_with(splits[0], (N_REPLICA, TOKENS, DW), 1.0, 6.0, ((0, 2), (1, 16)), (1, 2, 16, 2.0))
    key_cotangent = centred(splits[1], (N_REPLICA, TOKENS, KW), 0.005, 0.029907227, ((0, 2), (1, 16)))
    local_params = centred(splits[2], (N_REPLICA, DW, KW), 1.0, 6.0, ((0, 2), (1, 16)), jnp.float32)
    global_params = centred(splits[3], (DW, KW), 1.0, 6.0, ((0, 16),), jnp.float32)
    outer_momentum = centred(splits[4], (N_DP, DW // N_DP, KW), 0.5, 3.0, ((0, 16), (1, 2)), jnp.float32)
    adam_first = centred(splits[5], (N_REPLICA, DW, KW), 0.3, 2.0, ((0, 2), (1, 16)), jnp.float32)
    adam_second = jnp.clip(jnp.exp(math.log(4.0) - 2.7725887 * jax.random.uniform(splits[6], (N_REPLICA, DW, KW), jnp.float32) ** shard_levels(splits[6], (N_REPLICA, DW, KW), ((0, 2), (1, 16)), -0.2, 0.2)), 0.25, 4.0)
    return {"layer_input": layer_input, "key_cotangent": key_cotangent, "local_params": local_params, "global_params": global_params, "outer_momentum": outer_momentum, "adam_first": adam_first, "adam_second": adam_second}


outer_mu = 0.9
outer_rate = 0.7
beta_one = 0.9
beta_two = 0.95
adam_eps = 1e-08
weight_decay = 0.1
inner_rate = 0.1
correct_one = 1.0 - 0.9 ** 50
correct_two = 1.0 - 0.95 ** 50

def reference(layer_input, key_cotangent, local_params, global_params, outer_momentum, adam_first, adam_second):
    gradients = []
    for replica_index in range(N_REPLICA):
        gradients.append(lax.dot_general(layer_input[replica_index], key_cotangent[replica_index], (((0,), (0,)), ((), ())), preferred_element_type=jnp.float32))
    gradient = jnp.stack(gradients)
    outer_grad = lax.optimization_barrier(jnp.mean(global_params[None] - local_params, axis=0))
    momentum_flat = outer_mu * outer_momentum.reshape(DW, KW) + outer_grad
    new_global = global_params - outer_rate * (outer_grad + outer_mu * momentum_flat)
    new_first = beta_one * adam_first + (1.0 - beta_one) * gradient
    new_second = beta_two * adam_second + (1.0 - beta_two) * gradient * gradient
    adam_step = new_first / correct_one / (jnp.sqrt(new_second / correct_two) + adam_eps) + weight_decay * local_params
    merged_params = (new_global[None] - inner_rate * adam_step).astype(jnp.bfloat16)
    new_momentum = momentum_flat.reshape(N_DP, DW // N_DP, KW)
    return (merged_params, new_global, new_momentum, new_first, new_second)
```

```python
import functools
import jax
import jax.numpy as jnp
from jax import lax
from jax.experimental import pallas as pl
from jax.experimental.pallas import tpu as pltpu
from jax.sharding import PartitionSpec as P

outer_mu = 0.9
outer_rate = 0.7
beta_one = 0.9
beta_two = 0.95
adam_eps = 1e-08
weight_decay = 0.1
inner_rate = 0.1
correct_one = 1.0 - 0.9**50
correct_two = 1.0 - 0.95**50

MESH = pl.DeviceIdType.MESH
HALVES = 2
NARROW_STAGES = 1


def bit_of(value, bit):
    return lax.rem(lax.div(value, 2**bit), 2)


def flipped(value, bit):
    return value + (1 - 2 * bit_of(value, bit)) * 2**bit


def free_bits(bits, done):
    return [b for b in range(bits) if b not in done]


def owner_at(bits, me, done, flip, slot):
    owner = 0
    for position, b in enumerate(free_bits(bits, done)):
        owner = owner + bit_of(slot, position) * 2**b
    for b in done:
        own = bit_of(me, b)
        owner = owner + (1 - own if b == flip else own) * 2**b
    return owner


def slot_of(bits, done, owner):
    slot = 0
    for position, b in enumerate(free_bits(bits, done)):
        slot = slot + bit_of(owner, b) * 2**position
    return slot


def place_of(order, owner):
    place = 0
    for position, b in enumerate(reversed(order)):
        place = place + bit_of(owner, b) * 2**position
    return place


def static_place(order, owner):
    return sum(((owner >> b) & 1) << position for position, b in enumerate(reversed(order)))


def orders_of(bits):
    rising = list(range(bits))
    swapped = rising[:2][::-1] + rising[2:]
    return [rising, swapped]


def kernel(
    n_dp, n_rep, splits, x_ref, c_ref, local_ref, global_ref, mom_ref, first_ref, second_ref,
    merged_ref, gnew_ref, mnew_ref, fnew_ref, snew_ref,
    grad, deltas, moms, mom_flat, outer, gathered, *rest,
):
    bits = n_dp.bit_length() - 1
    sends, recvs = rest[:bits], rest[bits:2 * bits]
    send_sem, recv_sem, gsend_sem, grecv_sem, rep_send, rep_recv, out_sem = rest[2 * bits:]
    rep, me = lax.axis_index("replica"), lax.axis_index("dp")
    rows0, width = local_ref.shape
    rows, cols = rows0 // splits, width // HALVES
    sub = mom_ref.shape[0]
    orders = orders_of(bits)

    barrier = pltpu.get_barrier_semaphore()
    for b in range(bits):
        pl.semaphore_signal(barrier, inc=1, device_id=(rep, flipped(me, b)), device_id_type=MESH)
    for d in range(1, n_rep):
        pl.semaphore_signal(
            barrier, inc=1, device_id=(lax.rem(rep + d, n_rep), me), device_id_type=MESH
        )
    pl.semaphore_wait(barrier, bits + n_rep - 1)

    rep_copies = []
    for d in range(1, n_rep):
        target = (lax.rem(rep + d, n_rep), me)
        for which, (src, dst) in enumerate(((local_ref, deltas), (mom_ref, moms))):
            copy = pltpu.make_async_remote_copy(
                src_ref=src, dst_ref=dst.at[d], send_sem=rep_send.at[d, which],
                recv_sem=rep_recv.at[d, which], device_id=target, device_id_type=MESH,
            )
            copy.start()
            rep_copies.append(copy)

    block = 128

    def product(i, carry):
        at = pl.ds(pl.multiple_of(i * block, block), block)
        grad[at, :] = lax.dot_general(
            x_ref[:, at], c_ref[...], (((0,), (0,)), ((), ())),
            preferred_element_type=jnp.float32,
        )
        return carry

    lax.fori_loop(0, x_ref.shape[1] // block, product, 0)

    def rows_of(owner, q):
        return pl.ds(pl.multiple_of(owner * rows0 + q * rows, 8), rows)

    def update_outer():
        for copy in rep_copies:
            copy.wait()
        moms[0] = mom_ref[...]
        deltas[0] = local_ref[...]
        for r in range(n_rep):
            mom_flat[r * sub:(r + 1) * sub, :] = moms[lax.rem(rep - r + n_rep, n_rep)]
        total = jnp.zeros(local_ref.shape, jnp.float32)
        for r in range(n_rep):
            total = total + (global_ref[...] - deltas[lax.rem(rep - r + n_rep, n_rep)])
        outer_grad = total / n_rep
        momentum = outer_mu * mom_flat[...] + outer_grad
        outer[...] = momentum
        gnew_ref[...] = global_ref[...] - outer_rate * (outer_grad + outer_mu * momentum)
        for r in range(n_rep):
            @pl.when(rep == r)
            def _():
                mnew_ref[...] = outer[r * sub:(r + 1) * sub, :]

    def steps(q, h):
        order = orders[h]
        ch = q * HALVES + h
        lanes = slice(h * cols, (h + 1) * cols)

        def halving(stage):
            b = order[stage]
            return pltpu.make_async_remote_copy(
                src_ref=sends[stage].at[ch], dst_ref=recvs[stage].at[ch],
                send_sem=send_sem.at[ch, stage], recv_sem=recv_sem.at[ch, stage],
                device_id=(rep, flipped(me, b)), device_id_type=MESH,
            )

        for stage in range(bits):
            done = order[:stage + 1]
            count = n_dp >> (stage + 1)
            b = order[stage]
            if stage:
                halving(stage - 1).wait()

            def fill(slot, carry):
                owner = owner_at(bits, me, done, b, slot)
                value = grad[rows_of(owner, q), lanes]
                if stage:
                    arrived = slot_of(bits, order[:stage], owner)
                    value = value + recvs[stage - 1][ch, arrived].astype(jnp.float32)
                sends[stage][ch, slot] = value.astype(sends[stage].dtype)
                return carry

            lax.fori_loop(0, count, fill, 0)
            halving(stage).start()

            if stage:
                def keep(slot, carry):
                    owner = owner_at(bits, me, done, None, slot)
                    arrived = slot_of(bits, order[:stage], owner)
                    at = rows_of(owner, q)
                    grad[at, lanes] = grad[at, lanes] + recvs[stage - 1][ch, arrived].astype(
                        jnp.float32
                    )
                    return carry

                lax.fori_loop(0, count, keep, 0)
            yield

        halving(bits - 1).wait()
        own = slice(q * rows, (q + 1) * rows)
        gradient = grad[rows_of(me, q), lanes] + recvs[bits - 1][ch, 0].astype(jnp.float32)
        first_new = beta_one * first_ref[own, lanes] + (1.0 - beta_one) * gradient
        second_new = beta_two * second_ref[own, lanes] + (1.0 - beta_two) * gradient * gradient
        fnew_ref[own, lanes] = first_new
        snew_ref[own, lanes] = second_new
        adam_step = (
            first_new / correct_one / (jnp.sqrt(second_new / correct_two) + adam_eps)
            + weight_decay * local_ref[own, lanes]
        )
        mine = place_of(order, me)
        gathered[ch, mine] = (gnew_ref[own, lanes] - inner_rate * adam_step).astype(jnp.bfloat16)

        for stage in range(bits):
            b = order[bits - 1 - stage]
            if stage:
                copy.wait()
            held = gathered.at[ch, pl.ds(lax.div(mine, 2**stage) * 2**stage, 2**stage)]
            copy = pltpu.make_async_remote_copy(
                src_ref=held, dst_ref=held,
                send_sem=gsend_sem.at[ch, stage], recv_sem=grecv_sem.at[ch, stage],
                device_id=(rep, flipped(me, b)), device_id_type=MESH,
            )
            copy.start()
            yield
        copy.wait()
        for owner in range(n_dp):
            pltpu.make_async_copy(
                gathered.at[ch, static_place(order, owner)],
                merged_ref.at[owner, own, lanes], out_sem.at[ch],
            ).start()
        yield

    chunks = [[steps(q, h) for h in range(HALVES)] for q in range(splits)]
    ticks = 2 * bits + 1
    for tick in range(ticks + splits - 1):
        first = [tick] if tick < splits else []
        for q in first + [q for q in range(splits) if q < tick and tick - q < ticks]:
            for chunk in chunks[q]:
                next(chunk)
        if tick == 0:
            update_outer()
    for q in range(splits):
        for h in range(HALVES):
            ch = q * HALVES + h
            pltpu.make_async_copy(
                gathered.at[ch],
                merged_ref.at[:, q * rows:(q + 1) * rows, h * cols:(h + 1) * cols],
                out_sem.at[ch],
            ).wait()


def per_device(
    layer_input, key_cotangent, local_params, global_params, outer_momentum, adam_first, adam_second
):
    n_dp, n_rep = lax.axis_size("dp"), lax.axis_size("replica")
    bits = n_dp.bit_length() - 1
    rows0, width = global_params.shape
    sub = outer_momentum.shape[1]
    features = layer_input.shape[2]
    splits = next(s for s in (4, 2, 1) if s == 1 or rows0 % (s * 16) == 0)
    channels = splits * HALVES
    rows, cols = rows0 // splits, width // HALVES
    f32 = jnp.float32

    def stage_buffers():
        return [
            pltpu.VMEM(
                (channels, n_dp >> (s + 1), rows, cols),
                jnp.bfloat16 if s < NARROW_STAGES else f32,
            )
            for s in range(bits)
        ]

    vmem = pl.BlockSpec(memory_space=pltpu.VMEM)
    merged, gnew, mnew, fnew, snew = pl.pallas_call(
        functools.partial(kernel, n_dp, n_rep, splits),
        out_shape=(
            jax.ShapeDtypeStruct((n_dp, rows0, width), jnp.bfloat16),
            jax.ShapeDtypeStruct((rows0, width), f32),
            jax.ShapeDtypeStruct((sub, width), f32),
            jax.ShapeDtypeStruct((rows0, width), f32),
            jax.ShapeDtypeStruct((rows0, width), f32),
        ),
        in_specs=[vmem] * 7,
        out_specs=(pl.BlockSpec(memory_space=pl.ANY),) + (vmem,) * 4,
        scratch_shapes=[
            pltpu.VMEM((features, width), f32),
            pltpu.VMEM((n_rep, rows0, width), f32),
            pltpu.VMEM((n_rep, sub, width), f32),
            pltpu.VMEM((rows0, width), f32),
            pltpu.VMEM((rows0, width), f32),
            pltpu.VMEM((channels, n_dp, rows, cols), jnp.bfloat16),
            *stage_buffers(),
            *stage_buffers(),
            pltpu.SemaphoreType.DMA((channels, bits)),
            pltpu.SemaphoreType.DMA((channels, bits)),
            pltpu.SemaphoreType.DMA((channels, bits)),
            pltpu.SemaphoreType.DMA((channels, bits)),
            pltpu.SemaphoreType.DMA((n_rep, 2)),
            pltpu.SemaphoreType.DMA((n_rep, 2)),
            pltpu.SemaphoreType.DMA((channels,)),
        ],
        compiler_params=pltpu.CompilerParams(
            collective_id=0, has_side_effects=True, vmem_limit_bytes=60 * 2**20
        ),
    )(
        layer_input[0], key_cotangent[0], local_params[0], global_params, outer_momentum[0],
        adam_first[0], adam_second[0],
    )
    return (merged.reshape(1, n_dp * rows0, width), gnew, mnew[None], fnew[None], snew[None])


def solution(mesh):
    placed = (
        P("replica", "dp", None),
        P("replica", "dp", None),
        P("replica", "dp", None),
        P("dp", None),
        P("dp", "replica", None),
        P("replica", "dp", None),
        P("replica", "dp", None),
    )
    return jax.shard_map(
        per_device,
        mesh=mesh,
        in_specs=placed,
        out_specs=(
            P("replica", None, None),
            P("dp", None),
            P("dp", "replica", None),
            P("replica", "dp", None),
            P("replica", "dp", None),
        ),
        check_vma=False,
    )
```

```python
import functools
import jax
import jax.numpy as jnp
from jax import lax
from jax.experimental import pallas as pl
from jax.experimental.pallas import tpu as pltpu
from jax.sharding import PartitionSpec as P

outer_mu = 0.9
outer_rate = 0.7
beta_one = 0.9
beta_two = 0.95
adam_eps = 1e-08
weight_decay = 0.1
inner_rate = 0.1
correct_one = 1.0 - 0.9**50
correct_two = 1.0 - 0.95**50

MESH = pl.DeviceIdType.MESH
HALVES = 2
NARROW_STAGES = 3
UNROLL = 8
SPLITS = (12, 6, 4, 2, 1)
LATE = ()
START = 2
STRIDE = 4
OUTER_AFTER = 1
BLOCK = 1024


def bit_of(value, bit):
    if isinstance(value, int):
        return (value >> bit) & 1
    return lax.rem(lax.div(value, 2**bit), 2)


def flipped(value, bit):
    return value + (1 - 2 * bit_of(value, bit)) * 2**bit


def free_bits(bits, done):
    return [b for b in range(bits) if b not in done]


def owner_at(bits, me, done, flip, slot):
    fixed = 0
    for b in done:
        own = bit_of(me, b)
        fixed = fixed + (1 - own if b == flip else own) * 2**b
    spread = 0
    for position, b in enumerate(free_bits(bits, done)):
        spread = spread + bit_of(slot, position) * 2**b
    return fixed + spread


def arrival_of(bits, done, last, slot):
    position = free_bits(bits, done[:-1]).index(done[-1])
    if isinstance(slot, int):
        above = slot >> position
    else:
        above = lax.div(slot, 2**position)
    below = slot - above * 2**position
    return above * 2 ** (position + 1) + below + last * 2**position


def place_of(order, owner):
    place = 0
    for position, b in enumerate(reversed(order)):
        place = place + bit_of(owner, b) * 2**position
    return place


def static_place(order, owner):
    return sum(((owner >> b) & 1) << position for position, b in enumerate(reversed(order)))


def orders_of(bits, late):
    rising = list(range(bits))
    low, high = rising[:2], rising[2:]
    if late:
        return [high + low, high + low[::-1]]
    return [low + high, low[::-1] + high]


def for_slots(count, body):
    if count <= UNROLL:
        for slot in range(count):
            body(slot)
    else:
        lax.fori_loop(0, count, lambda slot, carry: (body(slot), carry)[1], 0)


def kernel(
    n_dp, n_rep, splits, x_ref, c_ref, local_ref, global_ref, mom_ref, first_ref, second_ref,
    merged_ref, gnew_ref, mnew_ref, fnew_ref, snew_ref,
    grad, deltas, moms, mom_flat, outer, gathered, *rest,
):
    bits = n_dp.bit_length() - 1
    sends, recvs = rest[:bits], rest[bits:2 * bits]
    send_sem, recv_sem, gsend_sem, grecv_sem, rep_send, rep_recv, out_sem = rest[2 * bits:]
    rep, me = lax.axis_index("replica"), lax.axis_index("dp")
    rows0, width = local_ref.shape
    rows, cols = rows0 // splits, width // HALVES
    sub = mom_ref.shape[0]

    barrier = pltpu.get_barrier_semaphore()
    for b in range(bits):
        pl.semaphore_signal(barrier, inc=1, device_id=(rep, flipped(me, b)), device_id_type=MESH)
    for d in range(1, n_rep):
        pl.semaphore_signal(
            barrier, inc=1, device_id=(lax.rem(rep + d, n_rep), me), device_id_type=MESH
        )
    pl.semaphore_wait(barrier, bits + n_rep - 1)

    rep_copies = []
    for d in range(1, n_rep):
        target = (lax.rem(rep + d, n_rep), me)
        for which, (src, dst) in enumerate(((local_ref, deltas), (mom_ref, moms))):
            copy = pltpu.make_async_remote_copy(
                src_ref=src, dst_ref=dst.at[d], send_sem=rep_send.at[d, which],
                recv_sem=rep_recv.at[d, which], device_id=target, device_id_type=MESH,
            )
            copy.start()
            rep_copies.append(copy)

    block = BLOCK

    def product(i, carry):
        at = pl.ds(pl.multiple_of(i * block, block), block)
        grad[at, :] = lax.dot_general(
            x_ref[:, at], c_ref[...], (((0,), (0,)), ((), ())),
            preferred_element_type=jnp.float32,
        )
        return carry

    lax.fori_loop(0, x_ref.shape[1] // block, product, 0)

    def rows_of(owner, q):
        return pl.ds(pl.multiple_of(owner * rows0 + q * rows, 8), rows)

    def update_outer():
        for copy in rep_copies:
            copy.wait()
        moms[0] = mom_ref[...]
        deltas[0] = local_ref[...]
        for r in range(n_rep):
            mom_flat[r * sub:(r + 1) * sub, :] = moms[lax.rem(rep - r + n_rep, n_rep)]
        total = jnp.zeros(local_ref.shape, jnp.float32)
        for r in range(n_rep):
            total = total + (global_ref[...] - deltas[lax.rem(rep - r + n_rep, n_rep)])
        outer_grad = total / n_rep
        momentum = outer_mu * mom_flat[...] + outer_grad
        outer[...] = momentum
        gnew_ref[...] = global_ref[...] - outer_rate * (outer_grad + outer_mu * momentum)
        for r in range(n_rep):
            @pl.when(rep == r)
            def _():
                mnew_ref[...] = outer[r * sub:(r + 1) * sub, :]

    def steps(q, h):
        order = orders_of(bits, q in LATE)[h]
        ch = q * HALVES + h
        lanes = slice(h * cols, (h + 1) * cols)

        def halving(stage):
            b = order[stage]
            return pltpu.make_async_remote_copy(
                src_ref=sends[stage].at[ch], dst_ref=recvs[stage].at[ch],
                send_sem=send_sem.at[ch, stage], recv_sem=recv_sem.at[ch, stage],
                device_id=(rep, flipped(me, b)), device_id_type=MESH,
            )

        for stage in range(bits):
            done = order[:stage + 1]
            count = n_dp >> (stage + 1)
            b = order[stage]
            if stage:
                halving(stage - 1).wait()

            def fill(slot):
                owner = owner_at(bits, me, done, b, slot)
                value = grad[rows_of(owner, q), lanes]
                if stage:
                    arrived = arrival_of(bits, done, 1 - bit_of(me, b), slot)
                    value = value + recvs[stage - 1][ch, arrived].astype(jnp.float32)
                sends[stage][ch, slot] = value.astype(sends[stage].dtype)

            for_slots(count, fill)
            halving(stage).start()

            if stage:
                def keep(slot):
                    owner = owner_at(bits, me, done, None, slot)
                    arrived = arrival_of(bits, done, bit_of(me, b), slot)
                    at = rows_of(owner, q)
                    grad[at, lanes] = grad[at, lanes] + recvs[stage - 1][ch, arrived].astype(
                        jnp.float32
                    )

                for_slots(count, keep)
            yield

        halving(bits - 1).wait()
        own = slice(q * rows, (q + 1) * rows)
        gradient = grad[rows_of(me, q), lanes] + recvs[bits - 1][ch, 0].astype(jnp.float32)
        first_new = beta_one * first_ref[own, lanes] + (1.0 - beta_one) * gradient
        second_new = beta_two * second_ref[own, lanes] + (1.0 - beta_two) * gradient * gradient
        fnew_ref[own, lanes] = first_new
        snew_ref[own, lanes] = second_new
        adam_step = (
            first_new / correct_one / (jnp.sqrt(second_new / correct_two) + adam_eps)
            + weight_decay * local_ref[own, lanes]
        )
        mine = place_of(order, me)
        gathered[ch, mine] = (gnew_ref[own, lanes] - inner_rate * adam_step).astype(jnp.bfloat16)

        for stage in range(bits):
            b = order[bits - 1 - stage]
            if stage:
                copy.wait()
            held = gathered.at[ch, pl.ds(lax.div(mine, 2**stage) * 2**stage, 2**stage)]
            copy = pltpu.make_async_remote_copy(
                src_ref=held, dst_ref=held,
                send_sem=gsend_sem.at[ch, stage], recv_sem=grecv_sem.at[ch, stage],
                device_id=(rep, flipped(me, b)), device_id_type=MESH,
            )
            copy.start()
            yield
        copy.wait()
        for owner in range(n_dp):
            pltpu.make_async_copy(
                gathered.at[ch, static_place(order, owner)],
                merged_ref.at[owner, own, lanes], out_sem.at[ch],
            ).start()
        yield

    chunks = [[steps(q, h) for h in range(HALVES)] for q in range(splits)]
    due = sorted(
        (START * q + STRIDE * i, i > 0, q) for q in range(splits) for i in range(2 * bits + 1)
    )
    for count, (_, _, q) in enumerate(due):
        for chunk in chunks[q]:
            next(chunk)
        if count == OUTER_AFTER:
            update_outer()
    for q in range(splits):
        for h in range(HALVES):
            ch = q * HALVES + h
            pltpu.make_async_copy(
                gathered.at[ch],
                merged_ref.at[:, q * rows:(q + 1) * rows, h * cols:(h + 1) * cols],
                out_sem.at[ch],
            ).wait()


def finish_kernel(parts, *refs):
    count = len(parts)
    sources, results, held = refs[:count], refs[count:2 * count], refs[2 * count:3 * count]
    sem = refs[3 * count]
    pieces = []
    for index, cuts in enumerate(parts):
        size = sources[index].shape[0] // cuts
        for cut in range(cuts):
            pieces.append((index, slice(cut * size, (cut + 1) * size)))
    ins = [
        pltpu.make_async_copy(sources[i].at[at], held[i].at[at], sem.at[0, p])
        for p, (i, at) in enumerate(pieces)
    ]
    outs = [
        pltpu.make_async_copy(held[i].at[at], results[i].at[at], sem.at[1, p])
        for p, (i, at) in enumerate(pieces)
    ]
    for copy in ins:
        copy.start()
    for copy, onward in zip(ins, outs):
        copy.wait()
        onward.start()
    for copy in outs:
        copy.wait()


def finish(*arrays):
    parts = [8 if a.ndim == 3 and a.shape[0] % 8 == 0 else 1 for a in arrays]
    return pl.pallas_call(
        functools.partial(finish_kernel, parts),
        out_shape=tuple(jax.ShapeDtypeStruct(a.shape, a.dtype) for a in arrays),
        in_specs=[pl.BlockSpec(memory_space=pl.ANY)] * len(arrays),
        out_specs=tuple([pl.BlockSpec(memory_space=pl.ANY)] * len(arrays)),
        scratch_shapes=[pltpu.VMEM(a.shape, a.dtype) for a in arrays]
        + [pltpu.SemaphoreType.DMA((2, sum(parts)))],
    )(*arrays)


def per_device(
    layer_input, key_cotangent, local_params, global_params, outer_momentum, adam_first, adam_second
):
    n_dp, n_rep = lax.axis_size("dp"), lax.axis_size("replica")
    bits = n_dp.bit_length() - 1
    rows0, width = global_params.shape
    sub = outer_momentum.shape[1]
    features = layer_input.shape[2]
    splits = next(s for s in SPLITS if s == 1 or rows0 % (s * 16) == 0)
    channels = splits * HALVES
    rows, cols = rows0 // splits, width // HALVES
    f32 = jnp.float32

    def stage_buffers():
        return [
            pltpu.VMEM(
                (channels, n_dp >> (s + 1), rows, cols),
                jnp.bfloat16 if s < NARROW_STAGES else f32,
            )
            for s in range(bits)
        ]

    vmem = pl.BlockSpec(memory_space=pltpu.VMEM)
    results = pl.pallas_call(
        functools.partial(kernel, n_dp, n_rep, splits),
        out_shape=(
            jax.ShapeDtypeStruct((n_dp, rows0, width), jnp.bfloat16),
            jax.ShapeDtypeStruct((rows0, width), f32),
            jax.ShapeDtypeStruct((sub, width), f32),
            jax.ShapeDtypeStruct((rows0, width), f32),
            jax.ShapeDtypeStruct((rows0, width), f32),
        ),
        in_specs=[vmem] * 7,
        out_specs=(pl.BlockSpec(memory_space=pl.ANY),) + (vmem,) * 4,
        scratch_shapes=[
            pltpu.VMEM((features, width), f32),
            pltpu.VMEM((n_rep, rows0, width), f32),
            pltpu.VMEM((n_rep, sub, width), f32),
            pltpu.VMEM((rows0, width), f32),
            pltpu.VMEM((rows0, width), f32),
            pltpu.VMEM((channels, n_dp, rows, cols), jnp.bfloat16),
            *stage_buffers(),
            *stage_buffers(),
            pltpu.SemaphoreType.DMA((channels, bits)),
            pltpu.SemaphoreType.DMA((channels, bits)),
            pltpu.SemaphoreType.DMA((channels, bits)),
            pltpu.SemaphoreType.DMA((channels, bits)),
            pltpu.SemaphoreType.DMA((n_rep, 2)),
            pltpu.SemaphoreType.DMA((n_rep, 2)),
            pltpu.SemaphoreType.DMA((channels,)),
        ],
        compiler_params=pltpu.CompilerParams(
            collective_id=0, has_side_effects=True, vmem_limit_bytes=60 * 2**20
        ),
    )(
        layer_input[0], key_cotangent[0], local_params[0], global_params, outer_momentum[0],
        adam_first[0], adam_second[0],
    )
    merged, gnew, mnew, fnew, snew = finish(*results)
    return (merged.reshape(1, n_dp * rows0, width), gnew, mnew[None], fnew[None], snew[None])


def solution(mesh):
    placed = (
        P("replica", "dp", None),
        P("replica", "dp", None),
        P("replica", "dp", None),
        P("dp", None),
        P("dp", "replica", None),
        P("replica", "dp", None),
        P("replica", "dp", None),
    )
    return jax.shard_map(
        per_device,
        mesh=mesh,
        in_specs=placed,
        out_specs=(
            P("replica", None, None),
            P("dp", None),
            P("dp", "replica", None),
            P("replica", "dp", None),
            P("replica", "dp", None),
        ),
        check_vma=False,
    )
```
